256 devices in a mesh: days: 128 (over x, z, y), cols: 2 (over core).
Axes of the slice: x: 4, y: 4, z: 8, core: 2. Of those that a mesh axis runs over, the one named last changes fastest.
Arguments:
- cube: float32 [4096, 65536], P('days', 'cols'), may hold values from -800 to 800
- year_id: int32 [4096], P('days'), may hold values from 0 to 2, as said below
- parent: int32 [65536], P('cols'), may hold values from 0 to 511
Outputs:
- running: float32 [4096, 65536], P('days', 'cols')
- rollup: float32 [4096, 512], P('days', 'cols')
The draws below stay inside these ranges and needn't reach their ends.
Inputs may be any that keep to these rules, and one draw needn't show every extreme that they name: year_id never falls from one day to the next; every year of 0 to 2 has 1 to 3072 days.
All inputs are finite; a program needn't handle non-finite values.
Results may differ from the reference program's by a relative error of at most 0.00012.
Values sent between devices are 32-bit elements; how exact they have to be, the bound alone decides.
A program may use at most 128 MiB of HBM per device.

```python
import jax
import jax.numpy as jnp
from jax import lax

COLS = 65536
PARENTS = 512
YEARS = 3
DAYS = 4096


def draw_cube(key, part):
    first, second = jax.random.split(jax.random.fold_in(key, 7), 2)
    base = jnp.clip(jax.random.normal(first, (DAYS, COLS), jnp.float32), -6.0, 6.0)
    position = jnp.arange(DAYS, dtype=jnp.float32) / max(DAYS - 1, 1)
    rising = 1.0 + 2.0 * position
    column_scale = jnp.exp(jax.random.uniform(second, (COLS,), jnp.float32) * jnp.log(10.0))
    values = base * rising[:, None] * column_scale[None, :]
    return values.astype(jnp.float32)


def draw_year_id(key, part):
    first, second = jax.random.split(jax.random.fold_in(key, 11), 2)
    margin = max(DAYS // 8, 1)
    opening = jax.random.randint(first, (), margin, DAYS // 2, dtype=jnp.int32)
    upper = jnp.minimum(opening + DAYS // 2, DAYS - 1).astype(jnp.int32)
    closing = jax.random.randint(second, (), opening + margin, upper, dtype=jnp.int32)
    bounds = jnp.stack([opening, closing]).astype(jnp.int32)
    order = jnp.arange(DAYS, dtype=jnp.int32)
    passed = (order[:, None] >= bounds[None, :]).astype(jnp.int32)
    return jnp.minimum(jnp.sum(passed, axis=1), YEARS - 1).astype(jnp.int32)


def plant(result, stream_key, smallest, high):
    longest = result.shape.index(max(result.shape))
    spots = []
    for shift in (0, 1):
        where = [jax.random.randint(jax.random.fold_in(stream_key, axis), (), 0, length) for axis, length in enumerate(result.shape)]
        where[longest] = (where[longest] + shift) % result.shape[longest]
        spots.append(tuple(where))
    return result.at[spots[0]].set(smallest).at[spots[1]].set(high)


def setup_inputs(seed: int = 0) -> dict:
    key_of = jax.random.split(jax.random.key(seed), 4)
    cube = draw_cube(jax.random.fold_in(key_of[3], 71), 0)
    year_id = draw_year_id(jax.random.fold_in(key_of[3], 71), 0)
    parent = plant(jax.random.randint(key_of[2], (COLS,), 0, PARENTS), jax.random.fold_in(key_of[2], 1), 0, PARENTS - 1).astype(jnp.int32)
    return {"cube": cube, "year_id": year_id, "parent": parent}


def reference(cube, year_id, parent):
    previous = jnp.concatenate([year_id[:1] - 1, year_id[:-1]]).astype(jnp.int32)
    keeps = (year_id == previous).astype(jnp.float32)

    def advance(carry, items):
        row, keep = items
        carry = carry * keep + row
        return (carry, carry)
    start = jnp.zeros((cube.shape[1],), jnp.float32)
    _, ytd = lax.scan(advance, start, (cube, keeps))
    region = jax.ops.segment_sum(ytd.T, parent, num_segments=PARENTS).T
    scale = jnp.sqrt(jnp.sum(region * region) / (DAYS * PARENTS) + 1e-06)
    return (ytd / scale, region / scale)
```

```python
import functools

import jax
import jax.numpy as jnp
from jax import lax
from jax.experimental import pallas as pl
from jax.experimental.pallas import tpu as pltpu
from jax.sharding import Mesh
from jax.sharding import PartitionSpec as P

PARENTS = 512
NX, NZH, NZL, NY = 4, 4, 2, 4
GROUP = NX * NZL * NY
CHUNK = 1024
RUN = NZL * NY
F32 = jnp.float32
BF16 = jnp.bfloat16
MESH = pl.DeviceIdType.MESH


def ring(a, n):
    return min(a, n - a)


OFFSETS = sorted(
    [(dx, dz, dy) for dx in range(NX) for dz in range(NZL) for dy in range(NY)][1:],
    key=lambda o: -(ring(o[0], NX) + o[1] + ring(o[2], NY)),
)


def year_tile(years):
    rows = years.shape[1]
    t = lax.broadcasted_iota(jnp.int32, (rows, rows), 0)
    u = lax.broadcasted_iota(jnp.int32, (rows, rows), 1)
    column = jnp.sum(jnp.where(t == u, years.astype(F32), 0.0), axis=1, keepdims=True)
    return jnp.broadcast_to(column, (rows, 128))


def same(a, b):
    return jnp.where(a == b, 1.0, 0.0).astype(F32)


def exchange_kernel(
    entries,
    cube_hbm,
    year_hbm,
    parent_hbm,
    carry_out,
    rollup_out,
    inv_out,
    cube,
    year,
    parent,
    tails,
    ysend,
    yrs1,
    recv1,
    pre1,
    tot,
    ytot,
    recv2,
    yrs2,
    pre2,
    back,
    carry,
    acc,
    part,
    rpart,
    raw,
    rmsg,
    rr,
    rpre,
    rrun,
    rr3,
    rcin,
    qmsg,
    rq,
    load_sem,
    send_sem,
    recv_sem,
):
    days, width = cube.shape
    x, z, y, c = (lax.axis_index(a) for a in ("x", "z", "y", "c"))
    zh, zl = lax.div(z, NZL), lax.rem(z, NZL)
    xs = [lax.rem(x + d, NX) for d in range(NX)]
    zls = [lax.rem(zl + d, NZL) for d in range(NZL)]
    ys = [lax.rem(y + d, NY) for d in range(NY)]
    zhs = [lax.rem(zh + d, NZH) for d in range(NZH)]
    mine = (x * NZL + zl) * NY + y
    peers = [
        (
            {"x": xs[dx], "z": zh * NZL + zls[dz], "y": ys[dy], "c": c},
            (xs[dx] * NZL + zls[dz]) * NY + ys[dy],
        )
        for dx, dz, dy in OFFSETS
    ]
    far = [{"x": x, "z": zhs[d] * NZL + zl, "y": y, "c": c} for d in (2, 1, 3)]
    partner = {"x": x, "z": z, "y": y, "c": 1 - c}

    pieces = 8
    span = width // pieces
    small = [
        pltpu.make_async_copy(year_hbm, year, load_sem.at[pieces]),
        pltpu.make_async_copy(parent_hbm, parent, load_sem.at[pieces + 1]),
    ]
    loads = [
        pltpu.make_async_copy(
            cube_hbm.at[:, pl.ds(k * span, span)], cube.at[:, pl.ds(k * span, span)], load_sem.at[k]
        )
        for k in range(pieces)
    ]
    small[0].start()
    for load in loads:
        load.start()
    small[1].start()

    barrier = pltpu.get_barrier_semaphore()
    for device in [p[0] for p in peers] + far + [partner]:
        pl.semaphore_signal(barrier, inc=1, device_id=device, device_id_type=MESH)

    small[0].wait()
    ytile = year_tile(year[...])
    first, last = ytile[0:1], ytile[days - 1 : days]
    ysend[0:1, :] = first
    ysend[1:2, :] = last
    in_last = ytile == last
    in_first = same(ytile, first)

    for k in range(pieces):
        loads[k].wait()

        def tail_chunk(h, _):
            for s in range(8):
                begin = pl.multiple_of(h * CHUNK + s * 128, 128)
                rows = cube[:, pl.ds(begin, 128)]
                tails[h, s : s + 1, :] = jnp.sum(
                    jnp.where(in_last, rows, 0.0), axis=0, keepdims=True
                )
            return 0

        per = span // CHUNK
        lax.fori_loop(k * per, (k + 1) * per, tail_chunk, 0)

    pl.semaphore_wait(barrier, len(peers) + len(far) + 1)

    def send(src, dst, slot, device):
        copy = pltpu.make_async_remote_copy(
            src_ref=src,
            dst_ref=dst,
            send_sem=send_sem.at[slot],
            recv_sem=recv_sem.at[slot],
            device_id=device,
            device_id_type=MESH,
        )
        copy.start()

    def settle(ref, slot):
        copy = pltpu.make_async_remote_copy(
            src_ref=ref,
            dst_ref=ref,
            send_sem=send_sem.at[slot],
            recv_sem=recv_sem.at[slot],
            device_id=partner,
            device_id_type=MESH,
        )
        return copy

    others = len(peers)
    for device, index in peers:
        send(tails.at[index], recv1.at[mine], 0, device)
    for device, index in peers:
        send(ysend, yrs1.at[mine], 1, device)
    recv1[mine] = tails[mine]
    yrs1[mine] = ysend[...]

    small[1].wait()
    acc[...] = jnp.zeros_like(acc)
    half = PARENTS // 2

    def add_block(j, _):
        begin = pl.multiple_of(j * CHUNK, CHUNK)
        rows = cube[:, pl.ds(begin, CHUNK)]
        owner = parent[:, pl.ds(begin, CHUNK)]
        upper = owner >= half
        place = jnp.where(upper, owner - half, owner)
        low = jnp.where(upper, 0.0, rows)
        both = jnp.concatenate([low, rows - low], axis=0)
        head = both.astype(BF16)
        rest = (both - head.astype(F32)).astype(BF16)
        lhs = jnp.concatenate([head, rest], axis=0)
        targets = lax.broadcasted_iota(jnp.int32, (half, CHUNK), 0)
        onehot = jnp.where(targets == place, 1.0, 0.0).astype(BF16)
        acc[...] += lax.dot_general(
            lhs, onehot, (((1,), (1,)), ((), ())), preferred_element_type=F32
        )
        return 0

    lax.fori_loop(0, width // CHUNK, add_block, 0)
    for h in range(2):
        part[h] = (
            acc[h * days : (h + 1) * days, :] + acc[(h + 2) * days : (h + 3) * days, :]
        )
    send(part.at[1 - c], rpart, 2, partner)

    settle(recv1.at[pl.ds(0, others)], 0).wait_recv()
    settle(yrs1.at[pl.ds(0, others)], 1).wait_recv()
    for g in range(NX):
        run_first = yrs1[g * RUN, 0:1, :]
        total, total_year = None, None
        for k in range(RUN):
            d = g * RUN + k
            d_first, d_last = yrs1[d, 0:1, :], yrs1[d, 1:2, :]
            tile = recv1[d]
            if k == 0:
                pre1[d] = jnp.zeros_like(tile)
                total = tile
            else:
                pre1[d] = total * same(total_year, d_first)
                total = tile + total * same(total_year, d_last)
            total_year = d_last
        tot[g] = total
        ytot[g, 0:1, :] = run_first
        ytot[g, 1:2, :] = total_year
    for device in far:
        send(tot, recv2.at[zh], 3, device)
        send(ytot, yrs2.at[zh], 4, device)
    recv2[zh] = tot[...]
    yrs2[zh] = ytot[...]

    settle(rpart, 2).wait_recv()
    raw[...] = part[c] + rpart[...]
    order = lax.broadcasted_iota(jnp.int32, (days, 128), 0)

    def add_day(u, sums):
        row = raw[pl.ds(u, 1), :]
        year_u = jnp.sum(jnp.where(order == u, ytile, 0.0), axis=0, keepdims=True)
        keep = jnp.where(jnp.logical_and(ytile == year_u, order >= u), 1.0, 0.0)
        return sums[0] + keep * row[:, :128], sums[1] + keep * row[:, 128:]

    zero = jnp.zeros((days, 128), F32)
    loc = lax.fori_loop(0, days, add_day, (zero, zero))
    for i in range(2):
        rmsg[i : i + 1, :] = loc[i][days - 1 : days]
        rmsg[2 + i : 3 + i, :] = jnp.sum(loc[i] * in_first, axis=0, keepdims=True)
    rmsg[4:5, :] = first
    rmsg[5:6, :] = last
    rmsg[6:7, :] = jnp.sum(in_first, axis=0, keepdims=True)
    rmsg[7:8, :] = jnp.sum(loc[0] * loc[0] + loc[1] * loc[1], axis=0, keepdims=True)
    spot = pl.ds(pl.multiple_of(mine * 8, 8), 8)
    for device, index in peers:
        send(rmsg, rr.at[spot], 5, device)
    rr[spot, :] = rmsg[...]

    settle(recv2.at[pl.ds(0, NZH - 1)], 3).wait_recv()
    settle(yrs2.at[pl.ds(0, NZH - 1)], 4).wait_recv()
    total, total_year = None, None
    for g in range(NX):
        for h in range(NZH):
            r_first, r_last = yrs2[h, g, 0:1, :], yrs2[h, g, 1:2, :]
            tile = recv2[h, g]
            if total is None:
                pre2[g * NZH + h] = jnp.zeros_like(tile)
                total = tile
            else:
                pre2[g * NZH + h] = total * same(total_year, r_first)
                total = tile + total * same(total_year, r_last)
            total_year = r_last
    for g in range(NX):
        run_first = yrs1[g * RUN, 0:1, :]
        into = pre2[g * NZH + zh]
        for k in range(RUN):
            d = g * RUN + k
            back[d] = pre1[d] + into * same(yrs1[d, 0:1, :], run_first)
    for device, index in peers:
        send(back.at[index], carry.at[mine], 6, device)
    carry[mine] = back[mine]

    settle(rr.at[pl.ds(0, others * 8)], 5).wait_recv()

    def quantity(ref, row, n):
        return ref[pl.ds(row, n, stride=8), :]

    shape = (NX, RUN, 128)
    t3 = [quantity(rr, i, GROUP).reshape(shape) for i in range(2)]
    s3 = [quantity(rr, 2 + i, GROUP).reshape(shape) for i in range(2)]
    f3, l3, n3, q3 = (quantity(rr, i, GROUP).reshape(shape) for i in range(4, 8))
    rank = lax.broadcasted_iota(jnp.int32, shape, 1)
    pre = [jnp.zeros(shape, F32) for _ in range(2)]
    for k in range(RUN - 1):
        keep = jnp.where(jnp.logical_and(l3[:, k : k + 1] == f3, rank > k), 1.0, 0.0)
        pre = [pre[i] + keep * t3[i][:, k : k + 1] for i in range(2)]
    starts = same(f3, f3[:, 0:1])
    ends = same(l3, l3[:, RUN - 1 : RUN])
    energy = q3
    for i in range(2):
        energy += pre[i] * (2.0 * s3[i] + n3 * pre[i])
        rpre[:, i * 128 : (i + 1) * 128] = pre[i].reshape(GROUP, 128)
    rows = [jnp.sum(ends * t3[i], axis=1) for i in range(2)]
    rows += [jnp.sum(starts * (s3[i] + n3 * pre[i]), axis=1) for i in range(2)]
    rows += [f3[:, 0], l3[:, RUN - 1]]
    rows += [jnp.sum(starts * n3, axis=1), jnp.sum(energy, axis=1)]
    for g in range(NX):
        for i in range(8):
            rrun[g * 8 + i : g * 8 + i + 1, :] = rows[i][g : g + 1]
    spot3 = pl.ds(pl.multiple_of(zh * NX * 8, 8), NX * 8)
    for device in far:
        send(rrun, rr3.at[spot3], 7, device)
    rr3[spot3, :] = rrun[...]

    settle(rr3.at[pl.ds(0, (NZH - 1) * NX * 8)], 7).wait_recv()
    runs = NX * NZH
    t2 = [quantity(rr3, i, runs) for i in range(2)]
    u2 = [quantity(rr3, 2 + i, runs) for i in range(2)]
    f2, l2, n2, q2 = (quantity(rr3, i, runs) for i in range(4, 8))
    position = lax.broadcasted_iota(jnp.int32, (runs, 128), 0)
    turn = (position % NX) * NZH + position // NX
    cin = [jnp.zeros((runs, 128), F32) for _ in range(2)]
    for i in range(runs):
        when = (i % NX) * NZH + i // NX
        keep = jnp.where(jnp.logical_and(l2[i : i + 1] == f2, turn > when), 1.0, 0.0)
        cin = [cin[j] + keep * t2[j][i : i + 1] for j in range(2)]
    energy = q2
    for i in range(2):
        energy += cin[i] * (2.0 * u2[i] + n2 * cin[i])
        rcin[:, i * 128 : (i + 1) * 128] = cin[i]
    qmsg[...] = jnp.broadcast_to(jnp.sum(energy, axis=0, keepdims=True), (8, 128))
    send(qmsg, rq, 8, partner)

    own_run = rcin[pl.ds(zh * NX + x, 1), :]
    own_pre = rpre[pl.ds(mine, 1), :]
    opens = same(first, yrs1[x * RUN, 0:1, :])
    opens = jnp.concatenate([opens, opens], axis=1)
    own = own_pre + opens * own_run
    region = [loc[i] + in_first * own[:, i * 128 : (i + 1) * 128] for i in range(2)]

    settle(rq, 8).wait_recv()
    squares = jnp.sum(qmsg[...] + rq[...], axis=1, keepdims=True)
    inv = jnp.broadcast_to(lax.rsqrt(squares / entries + 1e-06), (8, 128))
    inv_out[...] = inv
    for i in range(2):
        rollup_out[:, i * 128 : (i + 1) * 128] = region[i] * inv[0:1]

    settle(carry.at[pl.ds(0, others)], 6).wait_recv()
    carry_out[...] = carry[...].reshape(GROUP * 8, 128)

    settle(recv1.at[pl.ds(0, others)], 0).wait_send()
    settle(yrs1.at[pl.ds(0, others)], 1).wait_send()
    settle(rpart, 2).wait_send()
    settle(recv2.at[pl.ds(0, NZH - 1)], 3).wait_send()
    settle(yrs2.at[pl.ds(0, NZH - 1)], 4).wait_send()
    settle(rr.at[pl.ds(0, others * 8)], 5).wait_send()
    settle(carry.at[pl.ds(0, others)], 6).wait_send()
    settle(rr3.at[pl.ds(0, (NZH - 1) * NX * 8)], 7).wait_send()
    settle(rq, 8).wait_send()


def exchange(cube, year, parent, entries):
    days, width = cube.shape
    half = PARENTS // 2
    anywhere = pl.BlockSpec(memory_space=pl.ANY)
    vmem = pl.BlockSpec(memory_space=pltpu.VMEM)
    V = lambda *shape: pltpu.VMEM(shape, F32)
    return pl.pallas_call(
        functools.partial(exchange_kernel, entries),
        out_shape=(
            jax.ShapeDtypeStruct((GROUP * 8, 128), F32),
            jax.ShapeDtypeStruct((days, half), F32),
            jax.ShapeDtypeStruct((8, 128), F32),
        ),
        in_specs=[anywhere] * 3,
        out_specs=(vmem,) * 3,
        scratch_shapes=[
            V(days, width),
            pltpu.VMEM((1, days), jnp.int32),
            pltpu.VMEM((1, width), jnp.int32),
            V(GROUP, 8, 128),
            V(2, 128),
            V(GROUP, 2, 128),
            V(GROUP, 8, 128),
            V(GROUP, 8, 128),
            V(NX, 8, 128),
            V(NX, 2, 128),
            V(NZH, NX, 8, 128),
            V(NZH, NX, 2, 128),
            V(NX * NZH, 8, 128),
            V(GROUP, 8, 128),
            V(GROUP, 8, 128),
            V(4 * days, half),
            V(2, days, half),
            V(days, half),
            V(days, half),
            V(8, 128),
            V(GROUP * 8, 128),
            V(GROUP, half),
            V(NX * 8, 128),
            V(NZH * NX * 8, 128),
            V(NX * NZH, half),
            V(8, 128),
            V(8, 128),
            pltpu.SemaphoreType.DMA((10,)),
            pltpu.SemaphoreType.DMA((9,)),
            pltpu.SemaphoreType.DMA((9,)),
        ],
        compiler_params=pltpu.CompilerParams(
            collective_id=0, has_side_effects=True, vmem_limit_bytes=24 * 1024 * 1024
        ),
        name="exchange",
    )(cube, year, parent)


BLOCK = 2048


def finish_kernel(cube, year, carry, small, inv, running, rollup):
    days = cube.shape[0]
    ytile = year_tile(year[...])
    in_first = same(ytile, ytile[0:1])
    order = lax.broadcasted_iota(jnp.int32, (days, 128), 0)
    steps = [s for s in (1, 2, 4, 8, 16) if s < days]
    keeps = [
        jnp.where(jnp.logical_and(order >= s, pltpu.roll(ytile, s, 0) == ytile), 1.0, 0.0)
        for s in steps
    ]
    scale = inv[0:1, :]

    def column(k, _):
        at = pl.ds(pl.multiple_of(k * 128, 128), 128)
        rows = cube[:, at]
        for s, keep in zip(steps, keeps):
            rows = rows + keep * pltpu.roll(rows, s, 0)
        running[:, at] = (rows + in_first * carry[pl.ds(k, 1), :]) * scale
        return 0

    lax.fori_loop(0, BLOCK // 128, column, 0, unroll=2)
    rollup[...] = small[...]


def finish(cube, year, carry, small, inv):
    days, width = cube.shape
    whole = lambda a: pl.BlockSpec(a.shape, lambda k: (0, 0))
    return pl.pallas_call(
        finish_kernel,
        grid=(width // BLOCK,),
        out_shape=(
            jax.ShapeDtypeStruct(cube.shape, F32),
            jax.ShapeDtypeStruct(small.shape, F32),
        ),
        in_specs=[
            pl.BlockSpec((days, BLOCK), lambda k: (0, k)),
            whole(year),
            pl.BlockSpec((BLOCK // 128, 128), lambda k: (k, 0)),
            whole(small),
            whole(inv),
        ],
        out_specs=(pl.BlockSpec((days, BLOCK), lambda k: (0, k)), whole(small)),
        compiler_params=pltpu.CompilerParams(
            dimension_semantics=("arbitrary",), vmem_limit_bytes=16 * 1024 * 1024
        ),
        name="finish",
    )(cube, year, carry, small, inv)


def body(cube, year_id, parent):
    days = cube.shape[0]
    entries = days * NX * NZH * NZL * NY * PARENTS
    year = year_id.reshape(1, -1)
    carry, small, inv = exchange(cube, year, parent.reshape(1, -1), entries)
    return finish(cube, year, carry, small, inv)


def solution(mesh):
    finer = Mesh(mesh.devices.reshape(NX, NZH * NZL, NY, 2), ("x", "z", "y", "c"))
    days = ("x", "z", "y")
    return jax.shard_map(
        body,
        mesh=finer,
        in_specs=(P(days, "c"), P(days), P("c")),
        out_specs=(P(days, "c"), P(days, "c")),
        check_vma=False,
    )
```

```python
import functools

import jax
import jax.numpy as jnp
from jax import lax
from jax.experimental import pallas as pl
from jax.experimental.pallas import tpu as pltpu
from jax.sharding import Mesh
from jax.sharding import PartitionSpec as P

PARENTS = 512
NX, NZH, NZL, NY = 4, 4, 2, 4
GROUP = NX * NZL * NY
CHUNK = 1024
RUN = NZL * NY
F32 = jnp.float32
BF16 = jnp.bfloat16
MESH = pl.DeviceIdType.MESH


def ring(a, n):
    return min(a, n - a)


OFFSETS = sorted(
    [(dx, dz, dy) for dx in range(NX) for dz in range(NZL) for dy in range(NY)][1:],
    key=lambda o: -(ring(o[0], NX) + o[1] + ring(o[2], NY)),
)


def year_tile(years):
    rows = years.shape[1]
    t = lax.broadcasted_iota(jnp.int32, (rows, rows), 0)
    u = lax.broadcasted_iota(jnp.int32, (rows, rows), 1)
    column = jnp.sum(jnp.where(t == u, years.astype(F32), 0.0), axis=1, keepdims=True)
    return jnp.broadcast_to(column, (rows, 128))


def same(a, b):
    return jnp.where(a == b, 1.0, 0.0).astype(F32)


def exchange_kernel(
    entries,
    cube_hbm,
    year_hbm,
    parent_hbm,
    cube,
    carry_out,
    rollup_out,
    factors_out,
    year,
    parent,
    tails,
    ysend,
    yrs1,
    recv1,
    pre1,
    tot,
    ytot,
    recv2,
    yrs2,
    pre2,
    back,
    carry,
    acc,
    part,
    rpart,
    rmsg,
    rr,
    rpre,
    rrun,
    rr3,
    rcin,
    qmsg,
    rq,
    load_sem,
    send_sem,
    recv_sem,
):
    days, width = cube.shape
    x, z, y, c = (lax.axis_index(a) for a in ("x", "z", "y", "c"))
    zh, zl = lax.div(z, NZL), lax.rem(z, NZL)
    xs = [lax.rem(x + d, NX) for d in range(NX)]
    zls = [lax.rem(zl + d, NZL) for d in range(NZL)]
    ys = [lax.rem(y + d, NY) for d in range(NY)]
    zhs = [lax.rem(zh + d, NZH) for d in range(NZH)]
    mine = (x * NZL + zl) * NY + y
    peers = [
        (
            {"x": xs[dx], "z": zh * NZL + zls[dz], "y": ys[dy], "c": c},
            (xs[dx] * NZL + zls[dz]) * NY + ys[dy],
        )
        for dx, dz, dy in OFFSETS
    ]
    far = [{"x": x, "z": zhs[d] * NZL + zl, "y": y, "c": c} for d in (2, 1, 3)]
    partner = {"x": x, "z": z, "y": y, "c": 1 - c}

    pieces = 8
    span = width // pieces
    small = [
        pltpu.make_async_copy(year_hbm, year, load_sem.at[pieces]),
        pltpu.make_async_copy(parent_hbm, parent, load_sem.at[pieces + 1]),
    ]
    loads = [
        pltpu.make_async_copy(
            cube_hbm.at[:, pl.ds(k * span, span)], cube.at[:, pl.ds(k * span, span)], load_sem.at[k]
        )
        for k in range(pieces)
    ]
    small[0].start()
    for load in loads:
        load.start()
    small[1].start()

    barrier = pltpu.get_barrier_semaphore()
    for device in [p[0] for p in peers] + far + [partner]:
        pl.semaphore_signal(barrier, inc=1, device_id=device, device_id_type=MESH)

    small[0].wait()
    ytile = year_tile(year[...])
    first, last = ytile[0:1], ytile[days - 1 : days]
    ysend[0:1, :] = first
    ysend[1:2, :] = last
    in_first = same(ytile, first)
    ybyte = ytile.reshape(days // 8, 8, 128)
    order = lax.broadcasted_iota(jnp.int32, (days // 8, 8, 128), 1)
    keeps = [
        jnp.where(jnp.logical_and(order >= s, pltpu.roll(ybyte, s, 1) == ybyte), 1.0, 0.0)
        for s in (1, 2, 4)
    ]
    joins = [same(ybyte[i], ybyte[i - 1, 7:8]) for i in range(1, days // 8)]

    for k in range(pieces):
        loads[k].wait()

        def tail_chunk(h, _):
            for s in range(8):
                begin = pl.multiple_of(h * CHUNK + s * 128, 128)
                rows = cube[:, pl.ds(begin, 128)].reshape(days // 8, 8, 128)
                for shift, keep in zip((1, 2, 4), keeps):
                    rows = rows + keep * pltpu.roll(rows, shift, 1)
                groups = [rows[0]]
                for i, join in enumerate(joins):
                    groups.append(rows[i + 1] + join * groups[-1][7:8])
                for i, group in enumerate(groups):
                    cube[i * 8 : i * 8 + 8, pl.ds(begin, 128)] = group
                tails[h, s : s + 1, :] = groups[-1][7:8]
            return 0

        per = span // CHUNK
        lax.fori_loop(k * per, (k + 1) * per, tail_chunk, 0)

    pl.semaphore_wait(barrier, len(peers) + len(far) + 1)

    def send(src, dst, slot, device):
        copy = pltpu.make_async_remote_copy(
            src_ref=src,
            dst_ref=dst,
            send_sem=send_sem.at[slot],
            recv_sem=recv_sem.at[slot],
            device_id=device,
            device_id_type=MESH,
        )
        copy.start()

    def settle(ref, slot):
        return pltpu.make_async_remote_copy(
            src_ref=ref,
            dst_ref=ref,
            send_sem=send_sem.at[slot],
            recv_sem=recv_sem.at[slot],
            device_id=partner,
            device_id_type=MESH,
        )

    others = len(peers)
    for device, index in peers:
        send(tails.at[index], recv1.at[mine], 0, device)
    for device, index in peers:
        send(ysend, yrs1.at[mine], 1, device)
    recv1[mine] = tails[mine]
    yrs1[mine] = ysend[...]

    small[1].wait()
    acc[...] = jnp.zeros_like(acc)
    half = PARENTS // 2

    def add_block(j, _):
        begin = pl.multiple_of(j * CHUNK, CHUNK)
        rows = cube[:, pl.ds(begin, CHUNK)]
        owner = parent[:, pl.ds(begin, CHUNK)]
        upper = owner >= half
        place = jnp.where(upper, owner - half, owner)
        low = jnp.where(upper, 0.0, rows)
        both = jnp.concatenate([low, rows - low], axis=0)
        head = both.astype(BF16)
        rest = (both - head.astype(F32)).astype(BF16)
        lhs = jnp.concatenate([head, rest], axis=0)
        targets = lax.broadcasted_iota(jnp.int32, (half, CHUNK), 0)
        onehot = jnp.where(targets == place, 1.0, 0.0).astype(BF16)
        acc[...] += lax.dot_general(
            lhs, onehot, (((1,), (1,)), ((), ())), preferred_element_type=F32
        )
        return 0

    lax.fori_loop(0, width // CHUNK, add_block, 0)
    for h in range(2):
        part[h] = (
            acc[h * days : (h + 1) * days, :] + acc[(h + 2) * days : (h + 3) * days, :]
        )
    send(part.at[1 - c], rpart, 2, partner)

    settle(recv1.at[pl.ds(0, others)], 0).wait_recv()
    settle(yrs1.at[pl.ds(0, others)], 1).wait_recv()
    for g in range(NX):
        run_first = yrs1[g * RUN, 0:1, :]
        total, total_year = None, None
        for k in range(RUN):
            d = g * RUN + k
            d_first, d_last = yrs1[d, 0:1, :], yrs1[d, 1:2, :]
            tile = recv1[d]
            if k == 0:
                pre1[d] = jnp.zeros_like(tile)
                total = tile
            else:
                pre1[d] = total * same(total_year, d_first)
                total = tile + total * same(total_year, d_last)
            total_year = d_last
        tot[g] = total
        ytot[g, 0:1, :] = run_first
        ytot[g, 1:2, :] = total_year
    for device in far:
        send(tot, recv2.at[zh], 3, device)
        send(ytot, yrs2.at[zh], 4, device)
    recv2[zh] = tot[...]
    yrs2[zh] = ytot[...]

    settle(rpart, 2).wait_recv()
    loc = [part[c, :, i * 128 : i * 128 + 128] + rpart[:, i * 128 : i * 128 + 128] for i in range(2)]
    for i in range(2):
        rmsg[i : i + 1, :] = loc[i][days - 1 : days]
        rmsg[2 + i : 3 + i, :] = jnp.sum(loc[i] * in_first, axis=0, keepdims=True)
    rmsg[4:5, :] = first
    rmsg[5:6, :] = last
    rmsg[6:7, :] = jnp.sum(in_first, axis=0, keepdims=True)
    rmsg[7:8, :] = jnp.sum(loc[0] * loc[0] + loc[1] * loc[1], axis=0, keepdims=True)
    spot = pl.ds(pl.multiple_of(mine * 8, 8), 8)
    for device, index in peers:
        send(rmsg, rr.at[spot], 5, device)
    rr[spot, :] = rmsg[...]

    settle(recv2.at[pl.ds(0, NZH - 1)], 3).wait_recv()
    settle(yrs2.at[pl.ds(0, NZH - 1)], 4).wait_recv()
    total, total_year = None, None
    for g in range(NX):
        for h in range(NZH):
            r_first, r_last = yrs2[h, g, 0:1, :], yrs2[h, g, 1:2, :]
            tile = recv2[h, g]
            if total is None:
                pre2[g * NZH + h] = jnp.zeros_like(tile)
                total = tile
            else:
                pre2[g * NZH + h] = total * same(total_year, r_first)
                total = tile + total * same(total_year, r_last)
            total_year = r_last
    for g in range(NX):
        run_first = yrs1[g * RUN, 0:1, :]
        into = pre2[g * NZH + zh]
        for k in range(RUN):
            d = g * RUN + k
            back[d] = pre1[d] + into * same(yrs1[d, 0:1, :], run_first)
    for device, index in peers:
        send(back.at[index], carry.at[mine], 6, device)
    carry[mine] = back[mine]

    settle(rr.at[pl.ds(0, others * 8)], 5).wait_recv()

    def quantity(ref, row, n):
        return ref[pl.ds(row, n, stride=8), :]

    shape = (NX, RUN, 128)
    t3 = [quantity(rr, i, GROUP).reshape(shape) for i in range(2)]
    s3 = [quantity(rr, 2 + i, GROUP).reshape(shape) for i in range(2)]
    f3, l3, n3, q3 = (quantity(rr, i, GROUP).reshape(shape) for i in range(4, 8))
    rank = lax.broadcasted_iota(jnp.int32, shape, 1)
    pre = [jnp.zeros(shape, F32) for _ in range(2)]
    for k in range(RUN - 1):
        keep = jnp.where(jnp.logical_and(l3[:, k : k + 1] == f3, rank > k), 1.0, 0.0)
        pre = [pre[i] + keep * t3[i][:, k : k + 1] for i in range(2)]
    starts = same(f3, f3[:, 0:1])
    ends = same(l3, l3[:, RUN - 1 : RUN])
    energy = q3
    for i in range(2):
        energy += pre[i] * (2.0 * s3[i] + n3 * pre[i])
        rpre[:, i * 128 : (i + 1) * 128] = pre[i].reshape(GROUP, 128)
    rows = [jnp.sum(ends * t3[i], axis=1) for i in range(2)]
    rows += [jnp.sum(starts * (s3[i] + n3 * pre[i]), axis=1) for i in range(2)]
    rows += [f3[:, 0], l3[:, RUN - 1]]
    rows += [jnp.sum(starts * n3, axis=1), jnp.sum(energy, axis=1)]
    for g in range(NX):
        for i in range(8):
            rrun[g * 8 + i : g * 8 + i + 1, :] = rows[i][g : g + 1]
    spot3 = pl.ds(pl.multiple_of(zh * NX * 8, 8), NX * 8)
    for device in far:
        send(rrun, rr3.at[spot3], 7, device)
    rr3[spot3, :] = rrun[...]

    settle(rr3.at[pl.ds(0, (NZH - 1) * NX * 8)], 7).wait_recv()
    runs = NX * NZH
    t2 = [quantity(rr3, i, runs) for i in range(2)]
    u2 = [quantity(rr3, 2 + i, runs) for i in range(2)]
    f2, l2, n2, q2 = (quantity(rr3, i, runs) for i in range(4, 8))
    position = lax.broadcasted_iota(jnp.int32, (runs, 128), 0)
    turn = (position % NX) * NZH + position // NX
    cin = [jnp.zeros((runs, 128), F32) for _ in range(2)]
    for i in range(runs):
        when = (i % NX) * NZH + i // NX
        keep = jnp.where(jnp.logical_and(l2[i : i + 1] == f2, turn > when), 1.0, 0.0)
        cin = [cin[j] + keep * t2[j][i : i + 1] for j in range(2)]
    energy = q2
    for i in range(2):
        energy += cin[i] * (2.0 * u2[i] + n2 * cin[i])
        rcin[:, i * 128 : (i + 1) * 128] = cin[i]
    qmsg[...] = jnp.broadcast_to(jnp.sum(energy, axis=0, keepdims=True), (8, 128))
    send(qmsg, rq, 8, partner)

    own_run = rcin[pl.ds(zh * NX + x, 1), :]
    own_pre = rpre[pl.ds(mine, 1), :]
    opens = same(first, yrs1[x * RUN, 0:1, :])
    opens = jnp.concatenate([opens, opens], axis=1)
    own = own_pre + opens * own_run
    region = [loc[i] + in_first * own[:, i * 128 : (i + 1) * 128] for i in range(2)]

    settle(rq, 8).wait_recv()
    squares = jnp.sum(qmsg[...] + rq[...], axis=1, keepdims=True)
    inv = jnp.broadcast_to(lax.rsqrt(squares / entries + 1e-06), (8, 128))
    factors_out[0:8, :] = inv
    factors_out[8 : 8 + days, :] = in_first * inv[0:1]
    for i in range(2):
        rollup_out[:, i * 128 : (i + 1) * 128] = region[i] * inv[0:1]

    settle(carry.at[pl.ds(0, others)], 6).wait_recv()
    carry_out[...] = carry[...].reshape(GROUP * 8, 128)

    settle(recv1.at[pl.ds(0, others)], 0).wait_send()
    settle(yrs1.at[pl.ds(0, others)], 1).wait_send()
    settle(rpart, 2).wait_send()
    settle(recv2.at[pl.ds(0, NZH - 1)], 3).wait_send()
    settle(yrs2.at[pl.ds(0, NZH - 1)], 4).wait_send()
    settle(rr.at[pl.ds(0, others * 8)], 5).wait_send()
    settle(carry.at[pl.ds(0, others)], 6).wait_send()
    settle(rr3.at[pl.ds(0, (NZH - 1) * NX * 8)], 7).wait_send()
    settle(rq, 8).wait_send()


def exchange(cube, year, parent, entries):
    days, width = cube.shape
    half = PARENTS // 2
    hbm = pl.BlockSpec(memory_space=pltpu.HBM)
    vmem = pl.BlockSpec(memory_space=pltpu.VMEM)
    V = lambda *shape: pltpu.VMEM(shape, F32)
    return pl.pallas_call(
        functools.partial(exchange_kernel, entries),
        out_shape=(
            jax.ShapeDtypeStruct((days, width), F32),
            jax.ShapeDtypeStruct((GROUP * 8, 128), F32),
            jax.ShapeDtypeStruct((days, half), F32),
            jax.ShapeDtypeStruct((8 + days, 128), F32),
        ),
        in_specs=[hbm] * 3,
        out_specs=(vmem,) * 4,
        scratch_shapes=[
            pltpu.VMEM((1, days), jnp.int32),
            pltpu.VMEM((1, width), jnp.int32),
            V(GROUP, 8, 128),
            V(2, 128),
            V(GROUP, 2, 128),
            V(GROUP, 8, 128),
            V(GROUP, 8, 128),
            V(NX, 8, 128),
            V(NX, 2, 128),
            V(NZH, NX, 8, 128),
            V(NZH, NX, 2, 128),
            V(NX * NZH, 8, 128),
            V(GROUP, 8, 128),
            V(GROUP, 8, 128),
            V(4 * days, half),
            V(2, days, half),
            V(days, half),
            V(8, 128),
            V(GROUP * 8, 128),
            V(GROUP, half),
            V(NX * 8, 128),
            V(NZH * NX * 8, 128),
            V(NX * NZH, half),
            V(8, 128),
            V(8, 128),
            pltpu.SemaphoreType.DMA((10,)),
            pltpu.SemaphoreType.DMA((9,)),
            pltpu.SemaphoreType.DMA((9,)),
        ],
        compiler_params=pltpu.CompilerParams(
            collective_id=0, has_side_effects=True, vmem_limit_bytes=24 * 1024 * 1024
        ),
        name="exchange",
    )(*(pltpu.with_memory_space_constraint(a, pltpu.HBM) for a in (cube, year, parent)))


PIECES = 8


def finish_kernel(local, carry, small, factors, running, rollup, stage, sems):
    days, width = local.shape
    span = width // PIECES
    last = pltpu.make_async_copy(small, rollup, sems.at[PIECES])
    last.start()
    scale, opening = factors[0:1, :], factors[8 : 8 + days, :]
    copies = []
    for piece in range(PIECES):

        def column(k, _):
            at = pl.ds(pl.multiple_of(k * 128, 128), 128)
            stage[:, at] = local[:, at] * scale + opening * carry[pl.ds(k, 1), :]
            return 0

        per = span // 128
        lax.fori_loop(piece * per, (piece + 1) * per, column, 0, unroll=4)
        at = pl.ds(piece * span, span)
        copies.append(pltpu.make_async_copy(stage.at[:, at], running.at[:, at], sems.at[piece]))
        copies[-1].start()
    for copy in copies + [last]:
        copy.wait()


def finish(local, carry, small, factors):
    vmem = pl.BlockSpec(memory_space=pltpu.VMEM)
    hbm = pl.BlockSpec(memory_space=pltpu.HBM)
    return pl.pallas_call(
        finish_kernel,
        out_shape=(
            jax.ShapeDtypeStruct(local.shape, F32),
            jax.ShapeDtypeStruct(small.shape, F32),
        ),
        in_specs=[vmem] * 4,
        out_specs=(hbm, hbm),
        scratch_shapes=[
            pltpu.VMEM(local.shape, F32),
            pltpu.SemaphoreType.DMA((PIECES + 1,)),
        ],
        compiler_params=pltpu.CompilerParams(vmem_limit_bytes=16 * 1024 * 1024),
        name="finish",
    )(local, carry, small, factors)


def body(cube, year_id, parent):
    days = cube.shape[0]
    entries = days * NX * NZH * NZL * NY * PARENTS
    year = year_id.reshape(1, -1)
    local, carry, small, factors = exchange(cube, year, parent.reshape(1, -1), entries)
    return finish(local, carry, small, factors)


def solution(mesh):
    finer = Mesh(mesh.devices.reshape(NX, NZH * NZL, NY, 2), ("x", "z", "y", "c"))
    days = ("x", "z", "y")
    return jax.shard_map(
        body,
        mesh=finer,
        in_specs=(P(days, "c"), P(days), P("c")),
        out_specs=(P(days, "c"), P(days, "c")),
        check_vma=False,
    )
```

```python
import functools

import jax
import jax.numpy as jnp
from jax import lax
from jax.experimental import pallas as pl
from jax.experimental.pallas import tpu as pltpu
from jax.sharding import Mesh
from jax.sharding import PartitionSpec as P

PARENTS = 512
NX, NZH, NZL, NY = 4, 4, 2, 4
GROUP = NX * NZL * NY
CHUNK = 1024
PER = 16
RUN = NZL * NY
F32 = jnp.float32
BF16 = jnp.bfloat16
MESH = pl.DeviceIdType.MESH


def ring(a, n):
    return min(a, n - a)


OFFSETS = sorted(
    [(dx, dz, dy) for dx in range(NX) for dz in range(NZL) for dy in range(NY)][1:],
    key=lambda o: -(ring(o[0], NX) + o[1] + ring(o[2], NY)),
)


def year_tile(years):
    rows = years.shape[1]
    t = lax.broadcasted_iota(jnp.int32, (rows, rows), 0)
    u = lax.broadcasted_iota(jnp.int32, (rows, rows), 1)
    column = jnp.sum(jnp.where(t == u, years.astype(F32), 0.0), axis=1, keepdims=True)
    return jnp.broadcast_to(column, (rows, 128))


def same(a, b):
    return jnp.where(a == b, 1.0, 0.0).astype(F32)


def prefix_rows(rows, keeps, joins):
    days = rows.shape[0]
    rows = rows.reshape(days // 8, 8, 128)
    for shift, keep in zip((1, 2, 4), keeps):
        rows = rows + keep * pltpu.roll(rows, shift, 1)
    groups = [rows[0]]
    for i, join in enumerate(joins):
        groups.append(rows[i + 1] + join * groups[-1][7:8])
    return groups


def exchange_kernel(
    entries,
    cube_hbm,
    year_hbm,
    parent_hbm,
    cube,
    carry_out,
    rollup_out,
    factors_out,
    year,
    parent,
    tails,
    ysend,
    yrs1,
    recv1,
    pre1,
    tot,
    ytot,
    recv2,
    yrs2,
    pre2,
    back,
    carry,
    acc,
    part,
    rpart,
    rmsg,
    rr,
    rpre,
    rrun,
    rr3,
    rcin,
    qmsg,
    rq,
    load_sem,
    send_sem,
    recv_sem,
):
    days, width = cube.shape
    x, z, y, c = (lax.axis_index(a) for a in ("x", "z", "y", "c"))
    zh, zl = lax.div(z, NZL), lax.rem(z, NZL)
    xs = [lax.rem(x + d, NX) for d in range(NX)]
    zls = [lax.rem(zl + d, NZL) for d in range(NZL)]
    ys = [lax.rem(y + d, NY) for d in range(NY)]
    zhs = [lax.rem(zh + d, NZH) for d in range(NZH)]
    mine = (x * NZL + zl) * NY + y
    peers = [
        (
            {"x": xs[dx], "z": zh * NZL + zls[dz], "y": ys[dy], "c": c},
            (xs[dx] * NZL + zls[dz]) * NY + ys[dy],
        )
        for dx, dz, dy in OFFSETS
    ]
    far = [{"x": x, "z": zhs[d] * NZL + zl, "y": y, "c": c} for d in (2, 1, 3)]
    partner = {"x": x, "z": z, "y": y, "c": 1 - c}

    pieces = 8
    span = width // pieces
    small = [
        pltpu.make_async_copy(year_hbm, year, load_sem.at[pieces]),
        pltpu.make_async_copy(parent_hbm, parent, load_sem.at[pieces + 1]),
    ]
    loads = [
        pltpu.make_async_copy(
            cube_hbm.at[:, pl.ds(k * span, span)], cube.at[:, pl.ds(k * span, span)], load_sem.at[k]
        )
        for k in range(pieces)
    ]
    small[0].start()
    for load in loads:
        load.start()
    small[1].start()

    barrier = pltpu.get_barrier_semaphore()
    for device in [p[0] for p in peers] + far + [partner]:
        pl.semaphore_signal(barrier, inc=1, device_id=device, device_id_type=MESH)

    small[0].wait()
    ytile = year_tile(year[...])
    first, last = ytile[0:1], ytile[days - 1 : days]
    ysend[0:1, :] = first
    ysend[1:2, :] = last
    in_first = same(ytile, first)
    ybyte = ytile.reshape(days // 8, 8, 128)
    order = lax.broadcasted_iota(jnp.int32, (days // 8, 8, 128), 1)
    keeps = [
        jnp.where(jnp.logical_and(order >= s, pltpu.roll(ybyte, s, 1) == ybyte), 1.0, 0.0)
        for s in (1, 2, 4)
    ]
    joins = [same(ybyte[i], ybyte[i - 1, 7:8]) for i in range(1, days // 8)]

    in_last = ytile == last
    for k in range(pieces):
        loads[k].wait()

        def tail_chunk(h, _):
            for s in range(8):
                begin = pl.multiple_of(h * CHUNK + s * 128, 128)
                rows = jnp.where(in_last, cube[:, pl.ds(begin, 128)], 0.0)
                tails[h, s : s + 1, :] = jnp.sum(rows, axis=0, keepdims=True)
            return 0

        per = span // CHUNK
        lax.fori_loop(k * per, (k + 1) * per, tail_chunk, 0, unroll=2)

    pl.semaphore_wait(barrier, len(peers) + len(far) + 1)

    def send(src, dst, slot, device):
        copy = pltpu.make_async_remote_copy(
            src_ref=src,
            dst_ref=dst,
            send_sem=send_sem.at[slot],
            recv_sem=recv_sem.at[slot],
            device_id=device,
            device_id_type=MESH,
        )
        copy.start()

    def settle(ref, slot):
        return pltpu.make_async_remote_copy(
            src_ref=ref,
            dst_ref=ref,
            send_sem=send_sem.at[slot],
            recv_sem=recv_sem.at[slot],
            device_id=partner,
            device_id_type=MESH,
        )

    others = len(peers)
    for device, index in peers:
        send(tails.at[index], recv1.at[mine], 0, device)
    for device, index in peers:
        send(ysend, yrs1.at[mine], 1, device)
    recv1[mine] = tails[mine]
    yrs1[mine] = ysend[...]

    small[1].wait()
    acc[...] = jnp.zeros_like(acc)
    half = PARENTS // 2

    WIDE = 4096
    targets = lax.broadcasted_iota(jnp.int32, (half, WIDE), 0).astype(BF16)
    def add_block(j, _):
        begin = pl.multiple_of(j * WIDE, WIDE)
        rows = cube[:, pl.ds(begin, WIDE)]
        owner = parent[:, pl.ds(begin, WIDE)]
        upper = owner >= half
        place = jnp.where(upper, owner - half, owner).astype(F32).astype(BF16)
        low = jnp.where(upper, 0.0, rows)
        both = jnp.concatenate([low, rows - low], axis=0)
        head = both.astype(BF16)
        rest = (both - head.astype(F32)).astype(BF16)
        lhs = jnp.concatenate([head, rest], axis=0)
        onehot = jnp.where(targets == place, jnp.ones((), BF16), jnp.zeros((), BF16)).astype(jnp.float8_e4m3fn)
        acc[...] += lax.dot_general(
            lhs, onehot, (((1,), (1,)), ((), ())), preferred_element_type=F32
        )
        return 0

    lax.fori_loop(0, width // WIDE, add_block, 0)
    for h in range(2):
        part[h] = (
            acc[h * days : (h + 1) * days, :] + acc[(h + 2) * days : (h + 3) * days, :]
        )
    send(part.at[1 - c], rpart, 2, partner)

    settle(recv1.at[pl.ds(0, others)], 0).wait_recv()
    settle(yrs1.at[pl.ds(0, others)], 1).wait_recv()
    for g in range(NX):
        run_first = yrs1[g * RUN, 0:1, :]
        total, total_year = None, None
        for k in range(RUN):
            d = g * RUN + k
            d_first, d_last = yrs1[d, 0:1, :], yrs1[d, 1:2, :]
            tile = recv1[d]
            if k == 0:
                pre1[d] = jnp.zeros_like(tile)
                total = tile
            else:
                pre1[d] = total * same(total_year, d_first)
                total = tile + total * same(total_year, d_last)
            total_year = d_last
        tot[g] = total
        ytot[g, 0:1, :] = run_first
        ytot[g, 1:2, :] = total_year
    for device in far:
        send(tot, recv2.at[zh], 3, device)
        send(ytot, yrs2.at[zh], 4, device)
    recv2[zh] = tot[...]
    yrs2[zh] = ytot[...]

    settle(rpart, 2).wait_recv()
    loc = []
    for i in range(2):
        at = slice(i * 128, i * 128 + 128)
        loc.append(jnp.concatenate(prefix_rows(part[c, :, at] + rpart[:, at], keeps, joins), axis=0))
    for i in range(2):
        rmsg[i : i + 1, :] = loc[i][days - 1 : days]
        rmsg[2 + i : 3 + i, :] = jnp.sum(loc[i] * in_first, axis=0, keepdims=True)
    rmsg[4:5, :] = first
    rmsg[5:6, :] = last
    rmsg[6:7, :] = jnp.sum(in_first, axis=0, keepdims=True)
    rmsg[7:8, :] = jnp.sum(loc[0] * loc[0] + loc[1] * loc[1], axis=0, keepdims=True)
    spot = pl.ds(pl.multiple_of(mine * 8, 8), 8)
    for device, index in peers:
        send(rmsg, rr.at[spot], 5, device)
    rr[spot, :] = rmsg[...]

    def column(k, _):
        for s in range(PER):
            at = pl.ds(pl.multiple_of((k * PER + s) * 128, 128), 128)
            for i, group in enumerate(prefix_rows(cube[:, at], keeps, joins)):
                cube[i * 8 : i * 8 + 8, at] = group
        return 0

    lax.fori_loop(0, width // 128 // PER, column, 0)

    settle(recv2.at[pl.ds(0, NZH - 1)], 3).wait_recv()
    settle(yrs2.at[pl.ds(0, NZH - 1)], 4).wait_recv()
    total, total_year = None, None
    for g in range(NX):
        for h in range(NZH):
            r_first, r_last = yrs2[h, g, 0:1, :], yrs2[h, g, 1:2, :]
            tile = recv2[h, g]
            if total is None:
                pre2[g * NZH + h] = jnp.zeros_like(tile)
                total = tile
            else:
                pre2[g * NZH + h] = total * same(total_year, r_first)
                total = tile + total * same(total_year, r_last)
            total_year = r_last
    for g in range(NX):
        run_first = yrs1[g * RUN, 0:1, :]
        into = pre2[g * NZH + zh]
        for k in range(RUN):
            d = g * RUN + k
            back[d] = pre1[d] + into * same(yrs1[d, 0:1, :], run_first)
    for device, index in peers:
        send(back.at[index], carry.at[mine], 6, device)
    carry[mine] = back[mine]

    settle(rr.at[pl.ds(0, others * 8)], 5).wait_recv()

    def quantity(ref, row, n):
        return ref[pl.ds(row, n, stride=8), :]

    shape = (NX, RUN, 128)
    t3 = [quantity(rr, i, GROUP).reshape(shape) for i in range(2)]
    s3 = [quantity(rr, 2 + i, GROUP).reshape(shape) for i in range(2)]
    f3, l3, n3, q3 = (quantity(rr, i, GROUP).reshape(shape) for i in range(4, 8))
    rank = lax.broadcasted_iota(jnp.int32, shape, 1)
    pre = [jnp.zeros(shape, F32) for _ in range(2)]
    for k in range(RUN - 1):
        keep = jnp.where(jnp.logical_and(l3[:, k : k + 1] == f3, rank > k), 1.0, 0.0)
        pre = [pre[i] + keep * t3[i][:, k : k + 1] for i in range(2)]
    starts = same(f3, f3[:, 0:1])
    ends = same(l3, l3[:, RUN - 1 : RUN])
    energy = q3
    for i in range(2):
        energy += pre[i] * (2.0 * s3[i] + n3 * pre[i])
        rpre[:, i * 128 : (i + 1) * 128] = pre[i].reshape(GROUP, 128)
    rows = [jnp.sum(ends * t3[i], axis=1) for i in range(2)]
    rows += [jnp.sum(starts * (s3[i] + n3 * pre[i]), axis=1) for i in range(2)]
    rows += [f3[:, 0], l3[:, RUN - 1]]
    rows += [jnp.sum(starts * n3, axis=1), jnp.sum(energy, axis=1)]
    for g in range(NX):
        for i in range(8):
            rrun[g * 8 + i : g * 8 + i + 1, :] = rows[i][g : g + 1]
    spot3 = pl.ds(pl.multiple_of(zh * NX * 8, 8), NX * 8)
    for device in far:
        send(rrun, rr3.at[spot3], 7, device)
    rr3[spot3, :] = rrun[...]

    settle(rr3.at[pl.ds(0, (NZH - 1) * NX * 8)], 7).wait_recv()
    runs = NX * NZH
    t2 = [quantity(rr3, i, runs) for i in range(2)]
    u2 = [quantity(rr3, 2 + i, runs) for i in range(2)]
    f2, l2, n2, q2 = (quantity(rr3, i, runs) for i in range(4, 8))
    position = lax.broadcasted_iota(jnp.int32, (runs, 128), 0)
    turn = (position % NX) * NZH + position // NX
    cin = [jnp.zeros((runs, 128), F32) for _ in range(2)]
    for i in range(runs):
        when = (i % NX) * NZH + i // NX
        keep = jnp.where(jnp.logical_and(l2[i : i + 1] == f2, turn > when), 1.0, 0.0)
        cin = [cin[j] + keep * t2[j][i : i + 1] for j in range(2)]
    energy = q2
    for i in range(2):
        energy += cin[i] * (2.0 * u2[i] + n2 * cin[i])
        rcin[:, i * 128 : (i + 1) * 128] = cin[i]
    qmsg[...] = jnp.broadcast_to(jnp.sum(energy, axis=0, keepdims=True), (8, 128))
    send(qmsg, rq, 8, partner)

    own_run = rcin[pl.ds(zh * NX + x, 1), :]
    own_pre = rpre[pl.ds(mine, 1), :]
    opens = same(first, yrs1[x * RUN, 0:1, :])
    opens = jnp.concatenate([opens, opens], axis=1)
    own = own_pre + opens * own_run
    region = [loc[i] + in_first * own[:, i * 128 : (i + 1) * 128] for i in range(2)]

    settle(rq, 8).wait_recv()
    squares = jnp.sum(qmsg[...] + rq[...], axis=1, keepdims=True)
    inv = jnp.broadcast_to(lax.rsqrt(squares / entries + 1e-06), (8, 128))
    factors_out[0:8, :] = inv
    factors_out[8 : 8 + days, :] = in_first * inv[0:1]
    for i in range(2):
        rollup_out[:, i * 128 : (i + 1) * 128] = region[i] * inv[0:1]

    settle(carry.at[pl.ds(0, others)], 6).wait_recv()
    carry_out[...] = carry[...].reshape(GROUP * 8, 128)

    settle(recv1.at[pl.ds(0, others)], 0).wait_send()
    settle(yrs1.at[pl.ds(0, others)], 1).wait_send()
    settle(rpart, 2).wait_send()
    settle(recv2.at[pl.ds(0, NZH - 1)], 3).wait_send()
    settle(yrs2.at[pl.ds(0, NZH - 1)], 4).wait_send()
    settle(rr.at[pl.ds(0, others * 8)], 5).wait_send()
    settle(carry.at[pl.ds(0, others)], 6).wait_send()
    settle(rr3.at[pl.ds(0, (NZH - 1) * NX * 8)], 7).wait_send()
    settle(rq, 8).wait_send()


def exchange(cube, year, parent, entries):
    days, width = cube.shape
    half = PARENTS // 2
    hbm = pl.BlockSpec(memory_space=pltpu.HBM)
    vmem = pl.BlockSpec(memory_space=pltpu.VMEM)
    V = lambda *shape: pltpu.VMEM(shape, F32)
    return pl.pallas_call(
        functools.partial(exchange_kernel, entries),
        out_shape=(
            jax.ShapeDtypeStruct((days, width), F32),
            jax.ShapeDtypeStruct((GROUP * 8, 128), F32),
            jax.ShapeDtypeStruct((days, half), F32),
            jax.ShapeDtypeStruct((8 + days, 128), F32),
        ),
        in_specs=[hbm] * 3,
        out_specs=(vmem,) * 4,
        scratch_shapes=[
            pltpu.VMEM((1, days), jnp.int32),
            pltpu.VMEM((1, width), jnp.int32),
            V(GROUP, 8, 128),
            V(2, 128),
            V(GROUP, 2, 128),
            V(GROUP, 8, 128),
            V(GROUP, 8, 128),
            V(NX, 8, 128),
            V(NX, 2, 128),
            V(NZH, NX, 8, 128),
            V(NZH, NX, 2, 128),
            V(NX * NZH, 8, 128),
            V(GROUP, 8, 128),
            V(GROUP, 8, 128),
            V(4 * days, half),
            V(2, days, half),
            V(days, half),
            V(8, 128),
            V(GROUP * 8, 128),
            V(GROUP, half),
            V(NX * 8, 128),
            V(NZH * NX * 8, 128),
            V(NX * NZH, half),
            V(8, 128),
            V(8, 128),
            pltpu.SemaphoreType.DMA((10,)),
            pltpu.SemaphoreType.DMA((9,)),
            pltpu.SemaphoreType.DMA((9,)),
        ],
        compiler_params=pltpu.CompilerParams(
            collective_id=0, has_side_effects=True, vmem_limit_bytes=24 * 1024 * 1024
        ),
        name="exchange",
    )(*(pltpu.with_memory_space_constraint(a, pltpu.HBM) for a in (cube, year, parent)))


PIECES = 8


def finish_kernel(local, carry, small, factors, running, rollup, stage, sems):
    days, width = local.shape
    span = width // PIECES
    last = pltpu.make_async_copy(small, rollup, sems.at[PIECES])
    last.start()
    scale, opening = factors[0:1, :], factors[8 : 8 + days, :]
    copies = []
    for piece in range(PIECES):

        def column(k, _):
            at = pl.ds(pl.multiple_of(k * 128, 128), 128)
            stage[:, at] = local[:, at] * scale + opening * carry[pl.ds(k, 1), :]
            return 0

        per = span // 128
        lax.fori_loop(piece * per, (piece + 1) * per, column, 0, unroll=4)
        at = pl.ds(piece * span, span)
        copies.append(pltpu.make_async_copy(stage.at[:, at], running.at[:, at], sems.at[piece]))
        copies[-1].start()
    for copy in copies + [last]:
        copy.wait()


def finish(local, carry, small, factors):
    vmem = pl.BlockSpec(memory_space=pltpu.VMEM)
    hbm = pl.BlockSpec(memory_space=pltpu.HBM)
    return pl.pallas_call(
        finish_kernel,
        out_shape=(
            jax.ShapeDtypeStruct(local.shape, F32),
            jax.ShapeDtypeStruct(small.shape, F32),
        ),
        in_specs=[vmem] * 4,
        out_specs=(hbm, hbm),
        scratch_shapes=[
            pltpu.VMEM(local.shape, F32),
            pltpu.SemaphoreType.DMA((PIECES + 1,)),
        ],
        compiler_params=pltpu.CompilerParams(vmem_limit_bytes=16 * 1024 * 1024),
        name="finish",
    )(local, carry, small, factors)


def body(cube, year_id, parent):
    days = cube.shape[0]
    entries = days * NX * NZH * NZL * NY * PARENTS
    year = year_id.reshape(1, -1)
    local, carry, small, factors = exchange(cube, year, parent.reshape(1, -1), entries)
    return finish(local, carry, small, factors)


def solution(mesh):
    finer = Mesh(mesh.devices.reshape(NX, NZH * NZL, NY, 2), ("x", "z", "y", "c"))
    days = ("x", "z", "y")
    return jax.shard_map(
        body,
        mesh=finer,
        in_specs=(P(days, "c"), P(days), P("c")),
        out_specs=(P(days, "c"), P(days, "c")),
        check_vma=False,
    )
```
